32 devices in a mesh: rows: 16 (over z, y, core), cols: 2 (over x).
Axes of the slice: x: 2, y: 2, z: 4, core: 2. Of those that a mesh axis runs over, the one named last changes fastest.
Arguments:
- initial_field: float32 [16384, 4096], P(('rows', 'cols')), may hold values from -6 to 6
- diffusion: bfloat16 [16384, 4096], P(('rows', 'cols')), may hold values from 16 to 8192
Outputs:
- final_field: float32 [16384, 4096], P(('rows', 'cols'))
The draws below stay inside these ranges and needn't reach their ends.
All inputs are finite; a program needn't handle non-finite values.
Results may differ from the reference program's by a relative error of at most 0.0004.
Values may be sent and summed in bfloat16 or wider, within the bound.
A program may use at most 320 MiB of HBM per device.

```python
import math
import jax
import jax.numpy as jnp
from jax import lax

NX = 16384
ITERS = 2
NY = 4096


def draw_diffusion(key, part):
    tile_key, cell_key = jax.random.split(jax.random.fold_in(key, 7))
    tile_rows = (NX + 127) // 128
    tile_cols = (NY + 127) // 128
    lowest = 32.0
    highest = 2048.0
    tile_scale = jnp.exp(jax.random.uniform(tile_key, (tile_rows, tile_cols), jnp.float32, math.log(lowest), math.log(highest)))
    spread = jnp.exp(jax.random.uniform(cell_key, (NX, NY), jnp.float32, math.log(0.5), math.log(2.0)))
    tile_field = jnp.repeat(jnp.repeat(tile_scale, 128, axis=0)[:NX], 128, axis=1)[:, :NY]
    return (tile_field * spread).astype(jnp.bfloat16)


def level_of(rng, extent, shards, least, high):
    gain, own = 1.0, jax.random.fold_in(rng, 6)
    for position, parts in shards:
        draws = jnp.exp(jax.random.uniform(jax.random.fold_in(own, position), (parts,), jnp.float32, least / len(shards), high / len(shards)))
        gain = gain * jnp.repeat(draws, extent[position] // parts).reshape([-1 if axis == position else 1 for axis in range(len(extent))])
    return gain


def normal_values(key, shape, scale, reach, cuts=(), held_as=jnp.bfloat16):
    factor_of = level_of(key, shape, cuts, -0.22, 0.18) if cuts else 1.0
    array = jax.random.normal(key, shape, jnp.float32) * scale * factor_of
    return jnp.minimum(jnp.maximum(array, -reach), reach).astype(held_as)


def setup_inputs(seed: int = 0) -> dict:
    key_list = jax.random.split(jax.random.key(seed), 3)
    initial_field = normal_values(key_list[0], (NX, NY), 1.0, 6.0, ((0, 32),), jnp.float32)
    diffusion = draw_diffusion(jax.random.fold_in(key_list[2], 71), 0)
    return {"initial_field": initial_field, "diffusion": diffusion}


def lift_lines(values):
    return jnp.concatenate([values[1:], jnp.zeros_like(values[:1])], axis=0)


def lower_lines(values):
    return jnp.concatenate([jnp.zeros_like(values[:1]), values[:-1]], axis=0)


def reduce_solve(lower_band, upper_band, right_side):
    length = right_side.shape[0]
    batch = right_side.shape[1]
    if length == 1:
        return right_side
    halved = length // 2
    lower_pair = lower_band.reshape(halved, 2, batch)
    upper_pair = upper_band.reshape(halved, 2, batch)
    right_pair = right_side.reshape(halved, 2, batch)
    lower_even = lower_pair[:, 0]
    lower_odd = lower_pair[:, 1]
    upper_even = upper_pair[:, 0]
    upper_odd = upper_pair[:, 1]
    right_even = right_pair[:, 0]
    right_odd = right_pair[:, 1]
    divisor = 1.0 - lower_odd * upper_even - upper_odd * lift_lines(lower_even)
    coarse = reduce_solve(lower_odd * lower_even / divisor,
                          upper_odd * lift_lines(upper_even) / divisor,
                          (right_odd + lower_odd * right_even + upper_odd * lift_lines(right_even)) / divisor)
    even_values = right_even + lower_even * lower_lines(coarse) + upper_even * coarse
    return jnp.stack([even_values, coarse], axis=1).reshape(length, batch)


def solve_lines(coefficient, right_side):
    scaled = 1.0 + 2.0 * coefficient
    ratios = coefficient / scaled
    return reduce_solve(ratios, ratios, right_side / scaled)


def add_line_term(current, coefficient):
    return current + coefficient * (lower_lines(current) - 2.0 * current + lift_lines(current))


def solve_blocked(coefficient, right_side):
    length = right_side.shape[0]
    line_count = right_side.shape[1]
    block_cols = math.gcd(line_count, 256)
    blocks = line_count // block_cols

    def one_block(members):
        return solve_lines(members[0], members[1])

    coupling_blocks = coefficient.reshape(length, blocks, block_cols).transpose(1, 0, 2)
    right_blocks = right_side.reshape(length, blocks, block_cols).transpose(1, 0, 2)
    solved = lax.map(one_block, (coupling_blocks, right_blocks))
    return solved.transpose(1, 0, 2).reshape(length, line_count)


def reference(initial_field, diffusion):
    coupling = 0.5 * diffusion.astype(jnp.float32)
    coupling_turned = coupling.T
    current = initial_field
    for iteration in range(ITERS):
        right_turned = add_line_term(current.T, coupling_turned)
        middle = solve_blocked(coupling, right_turned.T)
        right_across = add_line_term(middle, coupling)
        current = solve_blocked(coupling_turned, right_across.T).T
    return current
```

```python
import functools

import jax
import jax.numpy as jnp
from jax import lax
from jax.experimental import pallas as pl
from jax.experimental.pallas import tpu as pltpu
from jax.sharding import PartitionSpec as P

ITERS = 2
LANES = 128
SUB = 8
PARTS = 5
Y_BLOCKS = 16


def row_slice(tiles, i):
    return pl.ds((i // SUB) * (tiles * SUB) + i % SUB, tiles, stride=SUB)


def eliminate(w, r, q, d):
    s = w + q
    m = 1.0 / (1.0 + s)
    return m, s * m, m * (r + d)


def summarise(steps, unroll, blocks, shape, fetch, keep=None):
    zero = jnp.zeros(shape, jnp.float32)
    one = jnp.ones(shape, jnp.float32)

    def body(g, carry):
        for u in range(unroll):
            step = g * unroll + u
            new = []
            for b in range(blocks):
                total_g, d, total_s, prod, m, q = carry[b]
                w, r = fetch(b, step)
                m, q, d = eliminate(w, r, q, d)
                if keep is not None:
                    keep(b, step, m)
                after = prod * m
                new.append((total_g + prod * d, d, total_s + prod * after, after, m, q))
            carry = tuple(new)
        return carry

    start = tuple((zero, zero, zero, one, zero, one) for _ in range(blocks))
    done = lax.fori_loop(0, steps // unroll, body, start)
    return [block[:PARTS] for block in done]


def merge(a, b):
    ga, da, sa, pa, ma = a
    gb, db, sb, pb, mb = b
    den = 1.0 / (1.0 - ma * sb)
    return (
        ga + pa * ((gb + sb * da) * den),
        db + pb * ((da + ma * gb) * den),
        sa + pa * pa * sb * den,
        pa * pb * den,
        mb + pb * pb * ma * den,
    )


def x_summary(rows, tiles, fetch, loc_ref, sum_ref):
    half = rows // 2
    blocks = summarise(half, 2, 2, (tiles, LANES), lambda b, step: fetch(b * half + step))
    for b in range(2):
        for part in range(PARTS):
            loc_ref[pl.ds((b * PARTS + part) * tiles, tiles), :] = blocks[b][part]
    merged = merge(blocks[0], blocks[1])
    for part in range(PARTS):
        sum_ref[pl.ds(part * tiles, tiles), :] = merged[part]


def first_kernel(rows, tiles, v_ref, w_ref, rhs_ref, loc_ref, sum_ref):
    shape = (tiles, LANES)
    lane = lax.broadcasted_iota(jnp.int32, shape, 1)
    tile = lax.broadcasted_iota(jnp.int32, shape, 0)

    def fetch(i):
        at = row_slice(tiles, i)
        v = v_ref[at, :]
        w = w_ref[at, :]
        turned = pltpu.roll(v, 1, 1)
        left = jnp.where(lane == 0, jnp.where(tile == 0, 0.0, pltpu.roll(turned, 1, 0)), turned)
        turned = pltpu.roll(v, LANES - 1, 1)
        right = jnp.where(
            lane == LANES - 1,
            jnp.where(tile == tiles - 1, 0.0, pltpu.roll(turned, tiles - 1, 0)),
            turned,
        )
        r = w * v + ((left - v) + (right - v))
        rhs_ref[at, :] = r
        return w, r

    x_summary(rows, tiles, fetch, loc_ref, sum_ref)


def outer_kernel(axes, sizes, all_ref, out_ref):
    me = lax.axis_index(axes[0]) * sizes[1] + lax.axis_index(axes[1])
    count = sizes[0] * sizes[1]

    def part(p, k):
        return all_ref[p, k]

    zero = jnp.zeros(all_ref.shape[2:], jnp.float32)

    def prefix(p, carry):
        dd, mm = carry
        g, d, s, pp, m = (part(p, k) for k in range(PARTS))
        den = 1.0 / (1.0 - mm * s)
        return d + pp * ((dd + mm * g) * den), m + pp * pp * mm * den

    def suffix(step, carry):
        gg, ss = carry
        p = count - 1 - step
        g, d, s, pp, m = (part(p, k) for k in range(PARTS))
        den = 1.0 / (1.0 - m * ss)
        return g + pp * ((gg + ss * d) * den), s + pp * pp * ss * den

    dd, mm = lax.fori_loop(0, me, prefix, (zero, zero))
    gg, ss = lax.fori_loop(0, count - 1 - me, suffix, (zero, zero))
    g, d, s, pp, m = (part(me, k) for k in range(PARTS))
    a11 = 1.0 - mm * s
    a22 = 1.0 - ss * m
    a12 = mm * pp
    a21 = ss * pp
    b1 = dd + mm * g
    b2 = gg + ss * d
    det = 1.0 / (a11 * a22 - a12 * a21)
    out_ref[0] = (a22 * b1 + a12 * b2) * det
    out_ref[1] = (a11 * b2 + a21 * b1) * det


def step_kernel(
    rows, tiles, last,
    w_ref, rhs_ref, loc_ref, outer_ref, out_ref, *rest,
):
    if last:
        m_ref, d_ref, wt_ref, rt_ref, small_ref = rest
    else:
        loc_out, sum_out, m_ref, d_ref, wt_ref, rt_ref, small_ref = rest
    half = rows // 2

    xl = outer_ref[0]
    xr = outer_ref[1]
    (ga, da, sa, pa, ma), (gb, db, sb, pb, mb) = [
        [loc_ref[pl.ds((b * PARTS + k) * tiles, tiles), :] for k in range(PARTS)] for b in range(2)
    ]
    den = 1.0 / (1.0 - ma * sb)
    first_b = (gb + pb * xr + sb * (da + pa * xl)) * den
    last_a = da + pa * xl + ma * first_b

    unroll = 2

    def x_forward(g, carry):
        for u in range(unroll):
            step = g * unroll + u
            new = []
            for b in range(2):
                q, d = carry[b]
                i = b * half + step
                at = row_slice(tiles, i)
                m, q, d = eliminate(w_ref[at, :], rhs_ref[at, :], q, d)
                to = pl.ds(i * tiles, tiles)
                m_ref[to, :] = m
                d_ref[to, :] = d
                new.append((q, d))
            carry = tuple(new)
        return carry

    one = jnp.ones((tiles, LANES), jnp.float32)
    lax.fori_loop(0, half // unroll, x_forward, ((one, xl), (one, last_a)))

    def x_backward(g, carry):
        for u in range(unroll):
            step = half - 1 - (g * unroll + u)
            new = []
            for b in range(2):
                i = b * half + step
                to = pl.ds(i * tiles, tiles)
                at = row_slice(tiles, i)
                x = d_ref[to, :] + m_ref[to, :] * carry[b]
                out_ref[at, :] = 2.0 * w_ref[at, :] * x - rhs_ref[at, :]
                new.append(x)
            carry = tuple(new)
        return carry

    lax.fori_loop(0, half // unroll, x_backward, (first_b, xr))

    row_tiles = rows // LANES
    kblocks = Y_BLOCKS
    length = tiles * LANES // kblocks
    region = length * row_tiles + SUB
    groups = LANES // SUB

    def natural(rt, t, k):
        return pl.ds(pl.multiple_of(((rt * groups + k) * tiles + t) * SUB, SUB), SUB)

    def turned_at(rt, t, k):
        j = t * LANES
        block = j // length
        s = j % length
        return pl.ds(
            pl.multiple_of(block * region + ((s // SUB + k) * row_tiles + rt) * SUB, SUB), SUB
        )

    def turn(source, target, from_at, to_at, rt, t):
        block = jnp.concatenate([source[from_at(rt, t, k), :] for k in range(groups)], axis=0)
        block = block.T
        for k in range(groups):
            target[to_at(rt, t, k), :] = block[k * SUB:(k + 1) * SUB, :]

    def turn_there(g, carry):
        rt = g // tiles
        t = g % tiles
        turn(out_ref, rt_ref, natural, turned_at, rt, t)
        turn(w_ref, wt_ref, natural, turned_at, rt, t)
        return carry

    lax.fori_loop(0, row_tiles * tiles, turn_there, 0)

    width = row_tiles * kblocks

    def y_slices(step):
        base = (step // SUB) * (row_tiles * SUB) + step % SUB
        return [pl.ds(base + rt * SUB, kblocks, stride=region) for rt in range(row_tiles)]

    def y_load(ref, step):
        return jnp.concatenate([ref[at, :] for at in y_slices(step)], axis=0)

    def y_keep(b, step, m):
        m_ref[pl.ds(step * width, width), :] = m

    (parts,) = summarise(
        length, 2, 1, (width, LANES), lambda b, step: (y_load(wt_ref, step), y_load(rt_ref, step)), y_keep
    )
    for k in range(PARTS):
        small_ref[pl.ds(k * width, width), :] = parts[k]

    def y_part(k, block):
        return small_ref[pl.ds(k * width + block, row_tiles, stride=kblocks), :]

    nothing = jnp.zeros((row_tiles, LANES), jnp.float32)
    before = [(nothing, nothing)]
    for block in range(kblocks - 1):
        dd, mm = before[-1]
        g, d, s, pp, m = (y_part(k, block) for k in range(PARTS))
        den = 1.0 / (1.0 - mm * s)
        before.append((d + pp * ((dd + mm * g) * den), m + pp * pp * mm * den))
    after = nothing
    for block in reversed(range(kblocks)):
        dd, mm = before[block]
        g = y_part(0, block)
        s = y_part(2, block)
        pp = y_part(3, block)
        head = (g + s * dd + pp * after) / (1.0 - s * mm)
        small_ref[pl.ds(PARTS * width + block, row_tiles, stride=kblocks), :] = dd + mm * head
        small_ref[pl.ds((PARTS + 1) * width + block, row_tiles, stride=kblocks), :] = after
        after = head

    y_unroll = 4

    def y_forward(g, d):
        for u in range(y_unroll):
            step = g * y_unroll + u
            to = pl.ds(step * width, width)
            d = m_ref[to, :] * (y_load(rt_ref, step) + d)
            d_ref[to, :] = d
        return d

    lax.fori_loop(0, length // y_unroll, y_forward, small_ref[pl.ds(PARTS * width, width), :])

    def y_backward(g, x):
        for u in range(y_unroll):
            step = length - 1 - (g * y_unroll + u)
            to = pl.ds(step * width, width)
            x = d_ref[to, :] + m_ref[to, :] * x
            for rt, at in enumerate(y_slices(step)):
                piece = x[rt * kblocks:(rt + 1) * kblocks, :]
                if last:
                    rt_ref[at, :] = piece
                else:
                    rt_ref[at, :] = 2.0 * wt_ref[at, :] * piece - rt_ref[at, :]
        return x

    lax.fori_loop(0, length // y_unroll, y_backward, small_ref[pl.ds((PARTS + 1) * width, width), :])

    def turn_back(g, carry):
        rt = 2 * (g // tiles)
        t = g % tiles
        for more in range(2 if row_tiles % 2 == 0 else 1):
            turn(rt_ref, out_ref, turned_at, natural, rt + more, t)
        return carry

    if row_tiles % 2 == 0:
        lax.fori_loop(0, row_tiles * tiles // 2, turn_back, 0)
    else:
        def turn_single(g, carry):
            turn(rt_ref, out_ref, turned_at, natural, g // tiles, g % tiles)
            return carry

        lax.fori_loop(0, row_tiles * tiles, turn_single, 0)

    if not last:
        def fetch(i):
            at = row_slice(tiles, i)
            return w_ref[at, :], out_ref[at, :]

        x_summary(rows, tiles, fetch, loc_out, sum_out)


def solution(mesh):
    axes = tuple(mesh.axis_names)
    sizes = tuple(mesh.shape[a] for a in axes)
    vmem = pl.BlockSpec(memory_space=pltpu.VMEM)
    params = pltpu.CompilerParams(vmem_limit_bytes=66 * 1000 * 1000)

    def local(initial_field, diffusion):
        rows, columns = initial_field.shape
        tiles = columns // LANES
        cells = rows * tiles

        def flat(values):
            values = values.reshape(rows // SUB, SUB, tiles, LANES)
            return values.transpose(0, 2, 1, 3).reshape(cells, LANES)

        def unflat(values):
            values = values.reshape(rows // SUB, tiles, SUB, LANES)
            return values.transpose(0, 2, 1, 3).reshape(rows, columns)

        def shape(count):
            return jax.ShapeDtypeStruct((count, LANES), jnp.float32)

        field = shape(cells)
        loc = shape(2 * PARTS * tiles)
        summary = shape(PARTS * tiles)
        w = 2.0 / flat(diffusion).astype(jnp.float32)
        rhs, local_summary, own = pl.pallas_call(
            functools.partial(first_kernel, rows, tiles),
            out_shape=(field, loc, summary),
            in_specs=[vmem] * 2,
            out_specs=[vmem] * 3,
            compiler_params=params,
            name="first",
        )(flat(initial_field), w)
        turned = cells + Y_BLOCKS * SUB
        width = rows // LANES * Y_BLOCKS
        for iteration in range(ITERS):
            last = iteration == ITERS - 1
            everyone = lax.all_gather(own, axes, axis=0, tiled=True)
            count = sizes[0] * sizes[1]
            chunk = min(tiles, 32)
            outer = pl.pallas_call(
                functools.partial(outer_kernel, axes, sizes),
                grid=(tiles // chunk,),
                out_shape=jax.ShapeDtypeStruct((2, tiles, LANES), jnp.float32),
                in_specs=[pl.BlockSpec((count, PARTS, chunk, LANES), lambda c: (0, 0, c, 0))],
                out_specs=pl.BlockSpec((2, chunk, LANES), lambda c: (0, c, 0)),
                name="outer",
            )(everyone.reshape(count, PARTS, tiles, LANES))
            result = pl.pallas_call(
                functools.partial(step_kernel, rows, tiles, last),
                out_shape=(field,) if last else (field, loc, summary),
                in_specs=[vmem] * 4,
                out_specs=[vmem] * (1 if last else 3),
                scratch_shapes=[
                    pltpu.VMEM((cells, LANES), jnp.float32),
                    pltpu.VMEM((cells, LANES), jnp.float32),
                    pltpu.VMEM((turned, LANES), jnp.float32),
                    pltpu.VMEM((turned, LANES), jnp.float32),
                    pltpu.VMEM(((PARTS + 2) * width, LANES), jnp.float32),
                ],
                compiler_params=params,
                name="last" if last else "middle",
            )(w, rhs, local_summary, outer)
            if last:
                return unflat(result[0])
            rhs, local_summary, own = result

    in_specs = (P(axes, None), P(axes, None))
    return jax.shard_map(local, mesh=mesh, in_specs=in_specs, out_specs=P(axes, None), check_vma=False)
```

```python
import functools

import jax
import jax.numpy as jnp
from jax import lax
from jax.experimental import pallas as pl
from jax.experimental.pallas import tpu as pltpu
from jax.sharding import PartitionSpec as P

ITERS = 2
LANES = 128
SUB = 8
PARTS = 5
Y_BLOCKS = 16


def row_slice(tiles, i):
    return pl.ds((i // SUB) * (tiles * SUB) + i % SUB, tiles, stride=SUB)


def eliminate(w, r, q, d):
    s = w + q
    m = 1.0 / (1.0 + s)
    return m, s * m, m * (r + d)


def summarise(steps, unroll, blocks, shape, fetch, keep=None):
    zero = jnp.zeros(shape, jnp.float32)
    one = jnp.ones(shape, jnp.float32)

    def body(g, carry):
        for u in range(unroll):
            step = g * unroll + u
            new = []
            for b in range(blocks):
                total_g, d, total_s, prod, m, q = carry[b]
                w, r = fetch(b, step)
                m, q, d = eliminate(w, r, q, d)
                if keep is not None:
                    keep(b, step, m)
                after = prod * m
                new.append((total_g + prod * d, d, total_s + prod * after, after, m, q))
            carry = tuple(new)
        return carry

    start = tuple((zero, zero, zero, one, zero, one) for _ in range(blocks))
    done = lax.fori_loop(0, steps // unroll, body, start)
    return [block[:PARTS] for block in done]


def merge(a, b):
    ga, da, sa, pa, ma = a
    gb, db, sb, pb, mb = b
    den = 1.0 / (1.0 - ma * sb)
    return (
        ga + pa * ((gb + sb * da) * den),
        db + pb * ((da + ma * gb) * den),
        sa + pa * pa * sb * den,
        pa * pb * den,
        mb + pb * pb * ma * den,
    )


def x_summary(rows, tiles, fetch, loc_ref, sum_ref):
    half = rows // 2
    blocks = summarise(half, 2, 2, (tiles, LANES), lambda b, step: fetch(b * half + step))
    for b in range(2):
        for part in range(PARTS):
            loc_ref[pl.ds((b * PARTS + part) * tiles, tiles), :] = blocks[b][part]
    merged = merge(blocks[0], blocks[1])
    for part in range(PARTS):
        sum_ref[pl.ds(part * tiles, tiles), :] = merged[part]


def first_kernel(rows, tiles, v_ref, w_ref, rhs_ref, loc_ref, sum_ref):
    shape = (tiles, LANES)
    lane = lax.broadcasted_iota(jnp.int32, shape, 1)
    tile = lax.broadcasted_iota(jnp.int32, shape, 0)

    def fetch(i):
        at = row_slice(tiles, i)
        v = v_ref[at, :]
        w = w_ref[at, :]
        turned = pltpu.roll(v, 1, 1)
        left = jnp.where(lane == 0, jnp.where(tile == 0, 0.0, pltpu.roll(turned, 1, 0)), turned)
        turned = pltpu.roll(v, LANES - 1, 1)
        right = jnp.where(
            lane == LANES - 1,
            jnp.where(tile == tiles - 1, 0.0, pltpu.roll(turned, tiles - 1, 0)),
            turned,
        )
        r = w * v + ((left - v) + (right - v))
        rhs_ref[at, :] = r
        return w, r

    x_summary(rows, tiles, fetch, loc_ref, sum_ref)


def outer_kernel(count, all_ref, out_ref, keep_ref):
    zero = jnp.zeros(all_ref.shape[2:], jnp.float32)

    def prefix(p, carry):
        dd, mm = carry
        out_ref[p, 0] = dd
        keep_ref[p] = mm
        g, d, s, pp, m = (all_ref[p, k] for k in range(PARTS))
        den = 1.0 / (1.0 - mm * s)
        return d + pp * ((dd + mm * g) * den), m + pp * pp * mm * den

    def suffix(step, after):
        p = count - 1 - step
        dd = out_ref[p, 0]
        mm = keep_ref[p]
        s = all_ref[p, 2]
        head = (all_ref[p, 0] + s * dd + all_ref[p, 3] * after) / (1.0 - s * mm)
        out_ref[p, 0] = dd + mm * head
        out_ref[p, 1] = after
        return head

    lax.fori_loop(0, count, prefix, (zero, zero))
    lax.fori_loop(0, count, suffix, zero)


def step_kernel(
    rows, tiles, last,
    w_ref, rhs_ref, loc_ref, outer_ref, out_ref, *rest,
):
    if last:
        m_ref, d_ref, wt_ref, rt_ref, small_ref = rest
    else:
        loc_out, sum_out, m_ref, d_ref, wt_ref, rt_ref, small_ref = rest
    half = rows // 2

    xl = outer_ref[0]
    xr = outer_ref[1]
    (ga, da, sa, pa, ma), (gb, db, sb, pb, mb) = [
        [loc_ref[pl.ds((b * PARTS + k) * tiles, tiles), :] for k in range(PARTS)] for b in range(2)
    ]
    den = 1.0 / (1.0 - ma * sb)
    first_b = (gb + pb * xr + sb * (da + pa * xl)) * den
    last_a = da + pa * xl + ma * first_b

    unroll = 2

    def x_forward(g, carry):
        for u in range(unroll):
            step = g * unroll + u
            new = []
            for b in range(2):
                q, d = carry[b]
                i = b * half + step
                at = row_slice(tiles, i)
                m, q, d = eliminate(w_ref[at, :], rhs_ref[at, :], q, d)
                to = pl.ds(i * tiles, tiles)
                m_ref[to, :] = m
                d_ref[to, :] = d
                new.append((q, d))
            carry = tuple(new)
        return carry

    one = jnp.ones((tiles, LANES), jnp.float32)
    lax.fori_loop(0, half // unroll, x_forward, ((one, xl), (one, last_a)))

    def x_backward(g, carry):
        for u in range(unroll):
            step = half - 1 - (g * unroll + u)
            new = []
            for b in range(2):
                i = b * half + step
                to = pl.ds(i * tiles, tiles)
                at = row_slice(tiles, i)
                x = d_ref[to, :] + m_ref[to, :] * carry[b]
                out_ref[at, :] = 2.0 * w_ref[at, :] * x - rhs_ref[at, :]
                new.append(x)
            carry = tuple(new)
        return carry

    lax.fori_loop(0, half // unroll, x_backward, (first_b, xr))

    row_tiles = rows // LANES
    kblocks = Y_BLOCKS
    length = tiles * LANES // kblocks
    region = length * row_tiles + SUB
    groups = LANES // SUB

    def natural(rt, t, k):
        return pl.ds(pl.multiple_of(((rt * groups + k) * tiles + t) * SUB, SUB), SUB)

    def turned_at(rt, t, k):
        j = t * LANES
        block = j // length
        s = j % length
        return pl.ds(
            pl.multiple_of(block * region + ((s // SUB + k) * row_tiles + rt) * SUB, SUB), SUB
        )

    def turn(source, target, from_at, to_at, rt, t):
        block = jnp.concatenate([source[from_at(rt, t, k), :] for k in range(groups)], axis=0)
        block = block.T
        for k in range(groups):
            target[to_at(rt, t, k), :] = block[k * SUB:(k + 1) * SUB, :]

    def turn_there(g, carry):
        rt = g // tiles
        t = g % tiles
        turn(out_ref, rt_ref, natural, turned_at, rt, t)
        turn(w_ref, wt_ref, natural, turned_at, rt, t)
        return carry

    lax.fori_loop(0, row_tiles * tiles, turn_there, 0)

    width = row_tiles * kblocks

    def y_slices(step):
        base = (step // SUB) * (row_tiles * SUB) + step % SUB
        return [pl.ds(base + rt * SUB, kblocks, stride=region) for rt in range(row_tiles)]

    def y_load(ref, step):
        return jnp.concatenate([ref[at, :] for at in y_slices(step)], axis=0)

    def y_keep(b, step, m):
        m_ref[pl.ds(step * width, width), :] = m

    (parts,) = summarise(
        length, 2, 1, (width, LANES), lambda b, step: (y_load(wt_ref, step), y_load(rt_ref, step)), y_keep
    )
    for k in range(PARTS):
        small_ref[pl.ds(k * width, width), :] = parts[k]

    def y_part(k, block):
        return small_ref[pl.ds(k * width + block, row_tiles, stride=kblocks), :]

    nothing = jnp.zeros((row_tiles, LANES), jnp.float32)
    before = [(nothing, nothing)]
    for block in range(kblocks - 1):
        dd, mm = before[-1]
        g, d, s, pp, m = (y_part(k, block) for k in range(PARTS))
        den = 1.0 / (1.0 - mm * s)
        before.append((d + pp * ((dd + mm * g) * den), m + pp * pp * mm * den))
    after = nothing
    for block in reversed(range(kblocks)):
        dd, mm = before[block]
        g = y_part(0, block)
        s = y_part(2, block)
        pp = y_part(3, block)
        head = (g + s * dd + pp * after) / (1.0 - s * mm)
        small_ref[pl.ds(PARTS * width + block, row_tiles, stride=kblocks), :] = dd + mm * head
        small_ref[pl.ds((PARTS + 1) * width + block, row_tiles, stride=kblocks), :] = after
        after = head

    y_unroll = 4

    def y_forward(g, d):
        for u in range(y_unroll):
            step = g * y_unroll + u
            to = pl.ds(step * width, width)
            d = m_ref[to, :] * (y_load(rt_ref, step) + d)
            d_ref[to, :] = d
        return d

    lax.fori_loop(0, length // y_unroll, y_forward, small_ref[pl.ds(PARTS * width, width), :])

    def y_backward(g, x):
        for u in range(y_unroll):
            step = length - 1 - (g * y_unroll + u)
            to = pl.ds(step * width, width)
            x = d_ref[to, :] + m_ref[to, :] * x
            for rt, at in enumerate(y_slices(step)):
                piece = x[rt * kblocks:(rt + 1) * kblocks, :]
                if last:
                    rt_ref[at, :] = piece
                else:
                    rt_ref[at, :] = 2.0 * wt_ref[at, :] * piece - rt_ref[at, :]
        return x

    lax.fori_loop(0, length // y_unroll, y_backward, small_ref[pl.ds((PARTS + 1) * width, width), :])

    def turn_back(g, carry):
        rt = 2 * (g // tiles)
        t = g % tiles
        for more in range(2 if row_tiles % 2 == 0 else 1):
            turn(rt_ref, out_ref, turned_at, natural, rt + more, t)
        return carry

    if row_tiles % 2 == 0:
        lax.fori_loop(0, row_tiles * tiles // 2, turn_back, 0)
    else:
        def turn_single(g, carry):
            turn(rt_ref, out_ref, turned_at, natural, g // tiles, g % tiles)
            return carry

        lax.fori_loop(0, row_tiles * tiles, turn_single, 0)

    if not last:
        def fetch(i):
            at = row_slice(tiles, i)
            return w_ref[at, :], out_ref[at, :]

        x_summary(rows, tiles, fetch, loc_out, sum_out)


def solution(mesh):
    axes = tuple(mesh.axis_names)
    sizes = tuple(mesh.shape[a] for a in axes)
    vmem = pl.BlockSpec(memory_space=pltpu.VMEM)
    params = pltpu.CompilerParams(vmem_limit_bytes=66 * 1000 * 1000)

    def local(initial_field, diffusion):
        rows, columns = initial_field.shape
        tiles = columns // LANES
        cells = rows * tiles

        def flat(values):
            values = values.reshape(rows // SUB, SUB, tiles, LANES)
            return values.transpose(0, 2, 1, 3).reshape(cells, LANES)

        def unflat(values):
            values = values.reshape(rows // SUB, tiles, SUB, LANES)
            return values.transpose(0, 2, 1, 3).reshape(rows, columns)

        def shape(count):
            return jax.ShapeDtypeStruct((count, LANES), jnp.float32)

        field = shape(cells)
        loc = shape(2 * PARTS * tiles)
        summary = shape(PARTS * tiles)
        w = 2.0 / flat(diffusion).astype(jnp.float32)
        rhs, local_summary, own = pl.pallas_call(
            functools.partial(first_kernel, rows, tiles),
            out_shape=(field, loc, summary),
            in_specs=[vmem] * 2,
            out_specs=[vmem] * 3,
            compiler_params=params,
            name="first",
        )(flat(initial_field), w)
        turned = cells + Y_BLOCKS * SUB
        width = rows // LANES * Y_BLOCKS
        for iteration in range(ITERS):
            last = iteration == ITERS - 1
            count = sizes[0] * sizes[1]
            share = tiles // count
            mine = own.reshape(PARTS, count, share, LANES).transpose(1, 0, 2, 3)
            everyone = lax.all_to_all(mine, axes, split_axis=0, concat_axis=0, tiled=True)
            solved = pl.pallas_call(
                functools.partial(outer_kernel, count),
                out_shape=jax.ShapeDtypeStruct((count, 2, share, LANES), jnp.float32),
                in_specs=[vmem],
                out_specs=vmem,
                scratch_shapes=[pltpu.VMEM((count, share, LANES), jnp.float32)],
                name="outer",
            )(everyone)
            outer = lax.all_to_all(solved, axes, split_axis=0, concat_axis=0, tiled=True)
            outer = outer.transpose(1, 0, 2, 3).reshape(2, tiles, LANES)
            result = pl.pallas_call(
                functools.partial(step_kernel, rows, tiles, last),
                out_shape=(field,) if last else (field, loc, summary),
                in_specs=[vmem] * 4,
                out_specs=[vmem] * (1 if last else 3),
                scratch_shapes=[
                    pltpu.VMEM((cells, LANES), jnp.float32),
                    pltpu.VMEM((cells, LANES), jnp.float32),
                    pltpu.VMEM((turned, LANES), jnp.float32),
                    pltpu.VMEM((turned, LANES), jnp.float32),
                    pltpu.VMEM(((PARTS + 2) * width, LANES), jnp.float32),
                ],
                compiler_params=params,
                name="last" if last else "middle",
            )(w, rhs, local_summary, outer)
            if last:
                return unflat(result[0])
            rhs, local_summary, own = result

    in_specs = (P(axes, None), P(axes, None))
    return jax.shard_map(local, mesh=mesh, in_specs=in_specs, out_specs=P(axes, None), check_vma=False)
```
